256 devices in a mesh: block: 4 (over y), span: 8 (over z), heads: 8 (over x, core).
Axes of the slice: x: 4, y: 4, z: 8, core: 2. Of those that a mesh axis runs over, the one named last changes fastest.
Arguments:
- fresh_keys: bfloat16 [32, 16384, 8, 128], P(None, ('block', 'span'), 'heads'), may hold values from -6 to 6
- fresh_values: bfloat16 [32, 16384, 8, 128], P(None, ('block', 'span'), 'heads'), may hold values from -6 to 6
- turn_angle: float32 [16384, 64], replicated, may hold values from -3.140625 to 3.140625
Outputs:
- stored_keys: bfloat16 [32, 16384, 8, 128], P(('block', 'span'), None, 'heads')
- stored_values: bfloat16 [32, 16384, 8, 128], P(('block', 'span'), None, 'heads')
- key_scale: float32 [32, 8, 128], P(('block', 'span'), 'heads')
The draws below stay inside these ranges and needn't reach their ends.
All inputs are finite; a program needn't handle non-finite values. Where the reference program divides by a largest or mean magnitude, that divisor is 1e-20 or more.
Results may differ from the reference program's by a relative error of at most 0.001.
Values may be sent and summed in bfloat16 or wider, within the bound.
A program may use at most 192 MiB of HBM per device.

```python
import jax
import jax.numpy as jnp

BATCH = 32
LENGTH = 16384
KV_HEADS = 8
HEAD_SIZE = 128
HALF_HEAD = 64


def steps_of(own_key, dims, split, low, top_value):
    loudness, own = 1.0, jax.random.fold_in(own_key, 6)
    for axis_at, blocks in split:
        draws = jnp.exp(jax.random.uniform(jax.random.fold_in(own, axis_at), (blocks,), jnp.float32, low / len(split), top_value / len(split)))
        loudness = loudness * jnp.repeat(draws, dims[axis_at] // blocks).reshape([-1 if axis == axis_at else 1 for axis in range(len(dims))])
    return loudness


def gaussian(rng, extent, scale, most, pieces=(), held_as=jnp.bfloat16):
    factor_of = steps_of(rng, extent, pieces, -0.22, 0.18) if pieces else 1.0
    result = jax.random.normal(rng, extent, jnp.float32) * scale * factor_of
    return jnp.minimum(jnp.maximum(result, -most), most).astype(held_as)


def setup_inputs(seed: int = 0) -> dict:
    splits = jax.random.split(jax.random.key(seed), 4)
    fresh_keys = gaussian(splits[0], (BATCH, LENGTH, KV_HEADS, HEAD_SIZE), 1.0, 6.0, ((1, 32), (2, 8)))
    fresh_values = gaussian(splits[1], (BATCH, LENGTH, KV_HEADS, HEAD_SIZE), 1.0, 6.0, ((1, 32), (2, 8)))
    turn_angle = jnp.clip(jax.random.uniform(splits[2], (LENGTH, HALF_HEAD), jnp.float32, -3.140625, 3.140625), -3.140625, 3.140625)
    return {"fresh_keys": fresh_keys, "fresh_values": fresh_values, "turn_angle": turn_angle}


def rotate_pairs(vectors, angle):
    half = vectors.shape[-1] // 2
    cosine, sine = jnp.cos(angle)[None, :, None, :], jnp.sin(angle)[None, :, None, :]
    first, second = vectors[..., :half], vectors[..., half:]
    return jnp.concatenate([first * cosine - second * sine, second * cosine + first * sine], axis=-1)


def keys_in_place(plain_keys, angle):
    wide_keys = plain_keys.astype(jnp.float32)
    return rotate_pairs(wide_keys, angle)


def reference(fresh_keys, fresh_values, turn_angle):
    turned_keys = keys_in_place(fresh_keys, turn_angle)
    key_scale = jnp.max(jnp.abs(turned_keys), axis=1)
    narrow_keys = (turned_keys / key_scale[:, None]).astype(jnp.bfloat16)
    stored_keys = narrow_keys
    stored_values = fresh_values
    return stored_keys, stored_values, key_scale
```

```python
import functools

import jax
import jax.numpy as jnp
from jax import lax
from jax.experimental import pallas as pl
from jax.experimental.pallas import tpu as pltpu
from jax.sharding import PartitionSpec as P

MESH = pl.DeviceIdType.MESH
DISTANCES = (4, 1, 2, 3)


def kernel(
    blocks, spans, rows,
    keys_ref, values_ref, angle_ref,
    out_keys, out_values, scale_ref,
    got_keys, angle, table, send_sem, recv_sem, own_sem,
):
    y, z, h = lax.axis_index("block"), lax.axis_index("span"), lax.axis_index("heads")
    core = lax.rem(h, 2)
    me = y * spans + z
    length = angle.shape[1]
    half = angle.shape[0]

    barrier = pltpu.get_barrier_semaphore()
    for step in range(1, blocks * spans):
        there = (lax.rem(y + step // spans, blocks), lax.rem(z + step % spans, spans), h)
        pl.semaphore_signal(barrier, inc=1, device_id=there, device_id_type=MESH)
    pl.semaphore_wait(barrier, blocks * spans - 1)

    def part(ref, index):
        return ref.at[pl.ds(pl.multiple_of(index * rows, rows), rows)]

    def copy(which, dy, dz):
        source, target = ((keys_ref, got_keys), (values_ref, out_values))[which]
        ty, tz = lax.rem(y + dy, blocks), lax.rem(z + dz + spans, spans)
        slot = which * blocks * spans + (dz % spans) * blocks + dy
        return pltpu.make_async_remote_copy(
            src_ref=part(source, ty * spans + tz),
            dst_ref=part(target, me),
            send_sem=send_sem.at[slot],
            recv_sem=recv_sem.at[slot],
            device_id=(ty, tz, h),
            device_id_type=MESH,
        )

    def arrival(which, dy, dz):
        source, target = ((keys_ref, got_keys), (values_ref, out_values))[which]
        fy, fz = lax.rem(y - dy + blocks, blocks), lax.rem(z - dz + spans, spans)
        slot = which * blocks * spans + dz * blocks + dy
        return pltpu.make_async_remote_copy(
            src_ref=part(source, me),
            dst_ref=part(target, fy * spans + fz),
            send_sem=send_sem.at[slot],
            recv_sem=recv_sem.at[slot],
            device_id=(fy, fz, h),
            device_id_type=MESH,
        )

    angle_copy = pltpu.make_async_copy(angle_ref, angle, own_sem.at[0])
    angle_copy.start()
    for which in range(2):
        for dy in (1, 3, 2):
            copy(which, dy, 0).start()
        for turn in range(blocks):
            for place, distance in enumerate(DISTANCES):
                for side, dz in enumerate((distance, -distance)):
                    if side and 2 * distance == spans:
                        continue
                    copy(which, lax.rem(2 * core + (turn + place + side), blocks), dz).start()
    own_keys = pltpu.make_async_copy(part(keys_ref, me), part(got_keys, me), own_sem.at[1])
    own_values = pltpu.make_async_copy(part(values_ref, me), part(out_values, me), own_sem.at[2])
    own_keys.start()
    own_values.start()
    angle_copy.wait()

    def fill(index, carry):
        start = pl.multiple_of(index * 128, 128)
        here = angle[:, pl.ds(start, 128)]
        both = jnp.concatenate([jnp.cos(here), jnp.sin(here)], axis=0)
        table[pl.ds(start, 128), :] = both.T
        return carry

    lax.fori_loop(0, length // 128, fill, 0)

    own_keys.wait()
    for slot in range(1, blocks * spans):
        arrival(0, slot % blocks, slot // blocks).wait_recv()

    first = lax.broadcasted_iota(jnp.int32, (128, 2 * half), 1) < half

    def turn_rows(index, most):
        at = pl.ds(pl.multiple_of(index * 128, 128), 128)
        wide = got_keys[at, :].astype(jnp.float32)
        here = table[at, :]
        swapped = pltpu.roll(here, half, 1)
        cosine = jnp.where(first, here, swapped)
        sine = jnp.where(first, -swapped, here)
        turned = wide * cosine + pltpu.roll(wide, half, 1) * sine
        table[at, :] = turned
        return jnp.maximum(most, jnp.max(jnp.abs(turned).reshape(16, 8, 2 * half), axis=0))

    most = lax.fori_loop(0, length // 128, turn_rows, jnp.zeros((8, 2 * half), jnp.float32))
    scale = jnp.max(most, axis=0, keepdims=True)
    scale_ref[...] = scale
    factor = 1.0 / scale

    def narrow_rows(index, carry):
        at = pl.ds(pl.multiple_of(index * 128, 128), 128)
        out_keys[at, :] = (table[at, :] * factor).astype(jnp.bfloat16)
        return carry

    lax.fori_loop(0, length // 128, narrow_rows, 0)

    own_values.wait()
    for slot in range(1, blocks * spans):
        arrival(1, slot % blocks, slot // blocks).wait_recv()
    for which in range(2):
        for slot in range(1, blocks * spans):
            arrival(which, slot % blocks, slot // blocks).wait_send()


def local(blocks, spans, fresh_keys, fresh_values, turn_angle):
    batch, rows, _, size = fresh_keys.shape
    length = batch * rows
    keys, values, scale = pl.pallas_call(
        functools.partial(kernel, blocks, spans, rows),
        out_shape=[
            jax.ShapeDtypeStruct((length, size), jnp.bfloat16),
            jax.ShapeDtypeStruct((length, size), jnp.bfloat16),
            jax.ShapeDtypeStruct((1, size), jnp.float32),
        ],
        in_specs=[pl.BlockSpec(memory_space=pltpu.HBM)] * 3,
        out_specs=[
            pl.BlockSpec(memory_space=pltpu.VMEM),
            pl.BlockSpec(memory_space=pl.ANY),
            pl.BlockSpec(memory_space=pltpu.VMEM),
        ],
        scratch_shapes=[
            pltpu.VMEM((length, size), jnp.bfloat16),
            pltpu.VMEM((size // 2, length), jnp.float32),
            pltpu.VMEM((length, size), jnp.float32),
            pltpu.SemaphoreType.DMA((2 * batch,)),
            pltpu.SemaphoreType.DMA((2 * batch,)),
            pltpu.SemaphoreType.DMA((3,)),
        ],
        compiler_params=pltpu.CompilerParams(
            collective_id=0, has_side_effects=True, vmem_limit_bytes=32 << 20
        ),
    )(
        *(
            pltpu.with_memory_space_constraint(array, pltpu.HBM)
            for array in (
                fresh_keys.reshape(length, size),
                fresh_values.reshape(length, size),
                turn_angle.T,
            )
        )
    )
    return (
        keys.reshape(1, length, 1, size),
        values.reshape(1, length, 1, size),
        scale.reshape(1, 1, size),
    )


def solution(mesh):
    blocks, spans = mesh.shape["block"], mesh.shape["span"]
    return jax.shard_map(
        functools.partial(local, blocks, spans),
        mesh=mesh,
        in_specs=(
            P(None, ("block", "span"), "heads", None),
            P(None, ("block", "span"), "heads", None),
            P(),
        ),
        out_specs=(
            P(("block", "span"), None, "heads", None),
            P(("block", "span"), None, "heads", None),
            P(("block", "span"), "heads", None),
        ),
        check_vma=False,
    )
```

```python
import functools

import jax
import jax.numpy as jnp
from jax import lax
from jax.experimental import pallas as pl
from jax.experimental.pallas import tpu as pltpu
from jax.sharding import PartitionSpec as P

MESH = pl.DeviceIdType.MESH
DISTANCES = (4, 1, 2, 3)


def kernel(
    blocks, spans, rows,
    keys_ref, values_ref, angle_ref,
    out_keys, out_values, scale_ref,
    keys, values, got_keys, angle, table, send_sem, recv_sem, own_sem,
):
    y, z, h = lax.axis_index("block"), lax.axis_index("span"), lax.axis_index("heads")
    core = lax.rem(h, 2)
    me = y * spans + z
    length = angle.shape[1]
    half = angle.shape[0]

    barrier = pltpu.get_barrier_semaphore()
    for step in range(1, blocks * spans):
        there = (lax.rem(y + step // spans, blocks), lax.rem(z + step % spans, spans), h)
        pl.semaphore_signal(barrier, inc=1, device_id=there, device_id_type=MESH)
    keys_in = pltpu.make_async_copy(keys_ref, keys, own_sem.at[0])
    values_in = pltpu.make_async_copy(values_ref, values, own_sem.at[1])
    angle_in = pltpu.make_async_copy(angle_ref, angle, own_sem.at[2])
    keys_in.start()
    values_in.start()
    pl.semaphore_wait(barrier, blocks * spans - 1)

    def part(ref, index):
        return ref.at[pl.ds(pl.multiple_of(index * rows, rows), rows)]

    def send(which, dy, dz):
        source, target = ((keys, got_keys), (values, out_values))[which]
        ty, tz = lax.rem(y + dy, blocks), lax.rem(z + dz + spans, spans)
        pltpu.make_async_remote_copy(
            src_ref=part(source, ty * spans + tz),
            dst_ref=part(target, me),
            send_sem=send_sem.at[which],
            recv_sem=recv_sem.at[which],
            device_id=(ty, tz, h),
            device_id_type=MESH,
        ).start()

    def others(which):
        source, target = ((keys, got_keys), (values, out_values))[which]
        count = (blocks * spans - 1) * rows
        return pltpu.make_async_remote_copy(
            src_ref=source.at[pl.ds(0, count)],
            dst_ref=target.at[pl.ds(0, count)],
            send_sem=send_sem.at[which],
            recv_sem=recv_sem.at[which],
            device_id=(lax.rem(y + 1, blocks), z, h),
            device_id_type=MESH,
        )

    for which, staged in enumerate((keys_in, values_in)):
        staged.wait()
        for turn in range(blocks):
            for place, distance in enumerate(DISTANCES):
                for side, dz in enumerate((distance, -distance)):
                    if side and 2 * distance == spans:
                        continue
                    send(which, lax.rem(2 * core + (turn + place + side), blocks), dz)
            if turn:
                send(which, turn, 0)
    own_keys = pltpu.make_async_copy(part(keys_ref, me), part(got_keys, me), own_sem.at[0])
    own_values = pltpu.make_async_copy(part(values_ref, me), part(out_values, me), own_sem.at[1])
    angle_in.start()
    own_keys.start()
    own_values.start()
    angle_in.wait()

    def fill(index, carry):
        start = pl.multiple_of(index * 128, 128)
        here = angle[:, pl.ds(start, 128)]
        both = jnp.concatenate([jnp.cos(here), jnp.sin(here)], axis=0)
        table[pl.ds(start, 128), :] = both.T
        return carry

    lax.fori_loop(0, length // 128, fill, 0)

    own_keys.wait()
    others(0).wait_recv()

    first = lax.broadcasted_iota(jnp.int32, (128, 2 * half), 1) < half

    def turn_rows(index, most):
        at = pl.ds(pl.multiple_of(index * 128, 128), 128)
        wide = got_keys[at, :].astype(jnp.float32)
        here = table[at, :]
        swapped = pltpu.roll(here, half, 1)
        cosine = jnp.where(first, here, swapped)
        sine = jnp.where(first, -swapped, here)
        turned = wide * cosine + pltpu.roll(wide, half, 1) * sine
        table[at, :] = turned
        return jnp.maximum(most, jnp.max(jnp.abs(turned).reshape(16, 8, 2 * half), axis=0))

    most = lax.fori_loop(0, length // 128, turn_rows, jnp.zeros((8, 2 * half), jnp.float32))
    scale = jnp.max(most, axis=0, keepdims=True)
    scale_ref[...] = scale
    factor = 1.0 / scale

    def narrow_rows(index, carry):
        at = pl.ds(pl.multiple_of(index * 128, 128), 128)
        out_keys[at, :] = (table[at, :] * factor).astype(jnp.bfloat16)
        return carry

    lax.fori_loop(0, length // 128, narrow_rows, 0)

    own_values.wait()
    others(0).wait_send()
    others(1).wait_send()
    others(1).wait_recv()


def put_out(keys, values, scale, out_keys, out_values, out_scale, sem):
    copies = [pltpu.make_async_copy(scale, out_scale, sem.at[0])]
    half = keys.shape[0] // 2
    for index, (source, target) in enumerate(((keys, out_keys), (values, out_values))):
        for piece in range(2):
            at = pl.ds(piece * half, half)
            copies.append(
                pltpu.make_async_copy(source.at[at], target.at[at], sem.at[1 + 2 * index + piece])
            )
    for one in copies:
        one.start()
    for one in copies:
        one.wait()


def local(blocks, spans, fresh_keys, fresh_values, turn_angle):
    batch, rows, _, size = fresh_keys.shape
    length = batch * rows
    shapes = [
        jax.ShapeDtypeStruct((length, size), jnp.bfloat16),
        jax.ShapeDtypeStruct((length, size), jnp.bfloat16),
        jax.ShapeDtypeStruct((1, size), jnp.float32),
    ]
    results = pl.pallas_call(
        functools.partial(kernel, blocks, spans, rows),
        out_shape=shapes,
        in_specs=[pl.BlockSpec(memory_space=pltpu.HBM)] * 3,
        out_specs=[
            pl.BlockSpec(memory_space=pltpu.VMEM),
            pl.BlockSpec(memory_space=pl.ANY),
            pl.BlockSpec(memory_space=pltpu.VMEM),
        ],
        scratch_shapes=[
            pltpu.VMEM((length, size), jnp.bfloat16),
            pltpu.VMEM((length, size), jnp.bfloat16),
            pltpu.VMEM((length, size), jnp.bfloat16),
            pltpu.VMEM((size // 2, length), jnp.float32),
            pltpu.VMEM((length, size), jnp.float32),
            pltpu.SemaphoreType.DMA((2,)),
            pltpu.SemaphoreType.DMA((2,)),
            pltpu.SemaphoreType.DMA((3,)),
        ],
        compiler_params=pltpu.CompilerParams(
            collective_id=0, has_side_effects=True, vmem_limit_bytes=40 << 20
        ),
    )(
        *(
            pltpu.with_memory_space_constraint(array, pltpu.HBM)
            for array in (
                fresh_keys.reshape(length, size),
                fresh_values.reshape(length, size),
                turn_angle.T,
            )
        )
    )
    keys, values, scale = pl.pallas_call(
        put_out,
        out_shape=shapes,
        in_specs=[pl.BlockSpec(memory_space=pl.ANY)] * 3,
        out_specs=[pl.BlockSpec(memory_space=pl.ANY)] * 3,
        scratch_shapes=[pltpu.SemaphoreType.DMA((5,))],
        compiler_params=pltpu.CompilerParams(vmem_limit_bytes=1 << 20),
    )(*results)
    return (
        keys.reshape(1, length, 1, size),
        values.reshape(1, length, 1, size),
        scale.reshape(1, 1, size),
    )


def solution(mesh):
    blocks, spans = mesh.shape["block"], mesh.shape["span"]
    return jax.shard_map(
        functools.partial(local, blocks, spans),
        mesh=mesh,
        in_specs=(
            P(None, ("block", "span"), "heads", None),
            P(None, ("block", "span"), "heads", None),
            P(),
        ),
        out_specs=(
            P(("block", "span"), None, "heads", None),
            P(("block", "span"), None, "heads", None),
            P(("block", "span"), "heads", None),
        ),
        check_vma=False,
    )
```

```python
import functools

import jax
import jax.numpy as jnp
from jax import lax
from jax.experimental import pallas as pl
from jax.experimental.pallas import tpu as pltpu
from jax.sharding import PartitionSpec as P

MESH = pl.DeviceIdType.MESH
DISTANCES = (4, 3, 2, 1)
AHEAD = ((1, 2, 3, 4), (1,))


def kernel(
    blocks, spans, rows,
    keys_ref, values_ref, angle_ref,
    out_keys, out_values, scale_ref,
    got_keys, angle, table, send_sem, recv_sem, own_sem, span_up, span_down, block_up, block_down,
):
    y, z, h = lax.axis_index("block"), lax.axis_index("span"), lax.axis_index("heads")
    core = lax.rem(h, 2)
    me = y * spans + z
    length = angle.shape[1]
    half = angle.shape[0]

    def part(ref, index):
        return ref.at[pl.ds(pl.multiple_of(index * rows, rows), rows)]

    def send(which, dy, dz):
        source, target = ((keys_ref, got_keys), (values_ref, out_values))[which]
        ty, tz = lax.rem(y + dy, blocks), lax.rem(z + dz + spans, spans)
        pltpu.make_async_remote_copy(
            src_ref=part(source, ty * spans + tz),
            dst_ref=part(target, me),
            send_sem=send_sem.at[which],
            recv_sem=recv_sem.at[which],
            device_id=(ty, tz, h),
            device_id_type=MESH,
        ).start()

    def others(which):
        source, target = ((keys_ref, got_keys), (values_ref, out_values))[which]
        count = (blocks * spans - 1) * rows
        return pltpu.make_async_remote_copy(
            src_ref=source.at[pl.ds(0, count)],
            dst_ref=target.at[pl.ds(0, count)],
            send_sem=send_sem.at[which],
            recv_sem=recv_sem.at[which],
            device_id=(lax.rem(y + 1, blocks), z, h),
            device_id_type=MESH,
        )

    def sides(distance):
        return (distance,) if 2 * distance == spans else (distance, -distance)

    def send_in_ring(which, distance):
        if distance in AHEAD[which]:
            for dz in sides(distance):
                send(which, 0, dz)

    angle_in = pltpu.make_async_copy(angle_ref, angle, own_sem.at[2])
    angle_in.start()

    span_next, span_last = (y, lax.rem(z + 1, spans), h), (y, lax.rem(z + spans - 1, spans), h)
    block_next, block_last = (lax.rem(y + 1, blocks), z, h), (lax.rem(y + blocks - 1, blocks), z, h)
    barrier = pltpu.get_barrier_semaphore()
    for neighbour in (span_next, span_last, block_next, block_last):
        pl.semaphore_signal(barrier, inc=1, device_id=neighbour, device_id_type=MESH)
    pl.semaphore_wait(barrier, 4)

    def pass_on(up, following, down, before):
        pl.semaphore_signal(up, inc=1, device_id=following, device_id_type=MESH)
        pl.semaphore_signal(down, inc=1, device_id=before, device_id_type=MESH)
        pl.semaphore_wait(up, 1)
        pl.semaphore_wait(down, 1)

    for which in range(2):
        send_in_ring(which, 1)
    for distance in range(2, spans // 2 + 1):
        pass_on(span_up, span_next, span_down, span_last)
        for which in range(2):
            send_in_ring(which, distance)
    for _ in range(blocks // 2):
        pass_on(block_up, block_next, block_down, block_last)

    for which in range(2):
        for turn in range(blocks):
            for place, distance in enumerate(DISTANCES):
                for side, dz in enumerate(sides(distance)):
                    step = 2 * core + (turn + place + side)
                    if distance not in AHEAD[which]:
                        send(which, lax.rem(step, blocks), dz)
                    elif turn < blocks - 1:
                        send(which, lax.rem(step, blocks - 1) + 1, dz)
            if turn:
                send(which, (1, 3, 2)[turn - 1], 0)
    own_keys = pltpu.make_async_copy(part(keys_ref, me), part(got_keys, me), own_sem.at[0])
    own_values = pltpu.make_async_copy(part(values_ref, me), part(out_values, me), own_sem.at[1])
    own_keys.start()
    own_values.start()
    angle_in.wait()

    def fill(index, carry):
        start = pl.multiple_of(index * 128, 128)
        here = angle[:, pl.ds(start, 128)]
        both = jnp.concatenate([jnp.cos(here), jnp.sin(here)], axis=0)
        table[pl.ds(start, 128), :] = both.T
        return carry

    lax.fori_loop(0, length // 128, fill, 0)

    own_keys.wait()
    others(0).wait_recv()

    first = lax.broadcasted_iota(jnp.int32, (128, 2 * half), 1) < half

    def turn_rows(index, most):
        at = pl.ds(pl.multiple_of(index * 128, 128), 128)
        wide = got_keys[at, :].astype(jnp.float32)
        here = table[at, :]
        swapped = pltpu.roll(here, half, 1)
        cosine = jnp.where(first, here, swapped)
        sine = jnp.where(first, -swapped, here)
        turned = wide * cosine + pltpu.roll(wide, half, 1) * sine
        table[at, :] = turned
        return jnp.maximum(most, jnp.max(jnp.abs(turned).reshape(16, 8, 2 * half), axis=0))

    most = lax.fori_loop(0, length // 128, turn_rows, jnp.zeros((8, 2 * half), jnp.float32))
    scale = jnp.max(most, axis=0, keepdims=True)
    scale_ref[...] = scale
    factor = 1.0 / scale

    def narrow_rows(index, carry):
        at = pl.ds(pl.multiple_of(index * 128, 128), 128)
        out_keys[at, :] = (table[at, :] * factor).astype(jnp.bfloat16)
        return carry

    lax.fori_loop(0, length // 128, narrow_rows, 0)

    own_values.wait()
    others(0).wait_send()
    others(1).wait_send()
    others(1).wait_recv()


def put_out(keys, values, scale, out_keys, out_values, out_scale, sem):
    copies = [pltpu.make_async_copy(scale, out_scale, sem.at[0])]
    half = keys.shape[0] // 2
    for index, (source, target) in enumerate(((keys, out_keys), (values, out_values))):
        for piece in range(2):
            at = pl.ds(piece * half, half)
            copies.append(
                pltpu.make_async_copy(source.at[at], target.at[at], sem.at[1 + 2 * index + piece])
            )
    for one in copies:
        one.start()
    for one in copies:
        one.wait()


def local(blocks, spans, fresh_keys, fresh_values, turn_angle):
    batch, rows, _, size = fresh_keys.shape
    length = batch * rows
    shapes = [
        jax.ShapeDtypeStruct((length, size), jnp.bfloat16),
        jax.ShapeDtypeStruct((length, size), jnp.bfloat16),
        jax.ShapeDtypeStruct((1, size), jnp.float32),
    ]
    results = pl.pallas_call(
        functools.partial(kernel, blocks, spans, rows),
        out_shape=shapes,
        in_specs=[pl.BlockSpec(memory_space=pltpu.HBM)] * 3,
        out_specs=[
            pl.BlockSpec(memory_space=pltpu.VMEM),
            pl.BlockSpec(memory_space=pl.ANY),
            pl.BlockSpec(memory_space=pltpu.VMEM),
        ],
        scratch_shapes=[
            pltpu.VMEM((length, size), jnp.bfloat16),
            pltpu.VMEM((size // 2, length), jnp.float32),
            pltpu.VMEM((length, size), jnp.float32),
            pltpu.SemaphoreType.DMA((2,)),
            pltpu.SemaphoreType.DMA((2,)),
            pltpu.SemaphoreType.DMA((3,)),
            *[pltpu.SemaphoreType.REGULAR] * 4,
        ],
        compiler_params=pltpu.CompilerParams(
            collective_id=0, has_side_effects=True, vmem_limit_bytes=32 << 20
        ),
    )(
        *(
            pltpu.with_memory_space_constraint(array, pltpu.HBM)
            for array in (
                fresh_keys.reshape(length, size),
                fresh_values.reshape(length, size),
                turn_angle.T,
            )
        )
    )
    keys, values, scale = pl.pallas_call(
        put_out,
        out_shape=shapes,
        in_specs=[pl.BlockSpec(memory_space=pl.ANY)] * 3,
        out_specs=[pl.BlockSpec(memory_space=pl.ANY)] * 3,
        scratch_shapes=[pltpu.SemaphoreType.DMA((5,))],
        compiler_params=pltpu.CompilerParams(vmem_limit_bytes=1 << 20),
    )(*results)
    return (
        keys.reshape(1, length, 1, size),
        values.reshape(1, length, 1, size),
        scale.reshape(1, 1, size),
    )


def solution(mesh):
    blocks, spans = mesh.shape["block"], mesh.shape["span"]
    return jax.shard_map(
        functools.partial(local, blocks, spans),
        mesh=mesh,
        in_specs=(
            P(None, ("block", "span"), "heads", None),
            P(None, ("block", "span"), "heads", None),
            P(),
        ),
        out_specs=(
            P(("block", "span"), None, "heads", None),
            P(("block", "span"), None, "heads", None),
            P(("block", "span"), "heads", None),
        ),
        check_vma=False,
    )
```

```python
import functools

import jax
import jax.numpy as jnp
from jax import lax
from jax.experimental import pallas as pl
from jax.experimental.pallas import tpu as pltpu
from jax.sharding import PartitionSpec as P

MESH = pl.DeviceIdType.MESH
DISTANCES = (3, 4, 2, 1)
AHEAD = ((1, 2, 3, 4), (1,))


def kernel(
    blocks, spans, rows,
    keys_ref, values_ref, angle_ref,
    out_keys, out_values, scale_ref,
    got_keys, angle, table, send_sem, recv_sem, own_sem, span_up, span_down, block_up, block_down,
):
    y, z, h = lax.axis_index("block"), lax.axis_index("span"), lax.axis_index("heads")
    core = lax.rem(h, 2)
    me = y * spans + z
    length = angle.shape[1]
    half = angle.shape[0]

    def part(ref, index):
        return ref.at[pl.ds(pl.multiple_of(index * rows, rows), rows)]

    def send(which, dy, dz):
        source, target = ((keys_ref, got_keys), (values_ref, out_values))[which]
        ty, tz = lax.rem(y + dy, blocks), lax.rem(z + dz + spans, spans)
        pltpu.make_async_remote_copy(
            src_ref=part(source, ty * spans + tz),
            dst_ref=part(target, me),
            send_sem=send_sem.at[which],
            recv_sem=recv_sem.at[which],
            device_id=(ty, tz, h),
            device_id_type=MESH,
        ).start()

    def others(which):
        source, target = ((keys_ref, got_keys), (values_ref, out_values))[which]
        count = (blocks * spans - 1) * rows
        return pltpu.make_async_remote_copy(
            src_ref=source.at[pl.ds(0, count)],
            dst_ref=target.at[pl.ds(0, count)],
            send_sem=send_sem.at[which],
            recv_sem=recv_sem.at[which],
            device_id=(lax.rem(y + 1, blocks), z, h),
            device_id_type=MESH,
        )

    def sides(distance):
        return (distance,) if 2 * distance == spans else (distance, -distance)

    def send_in_ring(which, distance):
        if distance in AHEAD[which]:
            for dz in sides(distance):
                send(which, 0, dz)

    angle_in = pltpu.make_async_copy(angle_ref, angle, own_sem.at[2])
    angle_in.start()

    span_next, span_last = (y, lax.rem(z + 1, spans), h), (y, lax.rem(z + spans - 1, spans), h)
    block_next, block_last = (lax.rem(y + 1, blocks), z, h), (lax.rem(y + blocks - 1, blocks), z, h)
    barrier = pltpu.get_barrier_semaphore()
    for neighbour in (span_next, span_last, block_next, block_last):
        pl.semaphore_signal(barrier, inc=1, device_id=neighbour, device_id_type=MESH)
    pl.semaphore_wait(barrier, 4)

    def pass_on(up, following, down, before):
        pl.semaphore_signal(up, inc=1, device_id=following, device_id_type=MESH)
        pl.semaphore_signal(down, inc=1, device_id=before, device_id_type=MESH)
        pl.semaphore_wait(up, 1)
        pl.semaphore_wait(down, 1)

    for which in range(2):
        send_in_ring(which, 1)
    for distance in range(2, spans // 2 + 1):
        pass_on(span_up, span_next, span_down, span_last)
        for which in range(2):
            send_in_ring(which, distance)
    for _ in range(blocks // 2):
        pass_on(block_up, block_next, block_down, block_last)

    for which in range(2):
        for turn in range(blocks):
            for place, distance in enumerate(DISTANCES):
                for side, dz in enumerate(sides(distance)):
                    step = 2 * core + (turn + place + side)
                    if distance not in AHEAD[which]:
                        send(which, lax.rem(step, blocks), dz)
                    elif turn < blocks - 1:
                        send(which, lax.rem(step, blocks - 1) + 1, dz)
            if turn:
                send(which, (1, 3, 2)[turn - 1], 0)
    own_keys = pltpu.make_async_copy(part(keys_ref, me), part(got_keys, me), own_sem.at[0])
    own_values = pltpu.make_async_copy(part(values_ref, me), part(out_values, me), own_sem.at[1])
    own_keys.start()
    own_values.start()
    angle_in.wait()

    def fill(index, carry):
        start = pl.multiple_of(index * 128, 128)
        here = angle[:, pl.ds(start, 128)]
        both = jnp.concatenate([jnp.cos(here), jnp.sin(here)], axis=0)
        table[pl.ds(start, 128), :] = both.T
        return carry

    lax.fori_loop(0, length // 128, fill, 0)

    own_keys.wait()
    others(0).wait_recv()

    first = lax.broadcasted_iota(jnp.int32, (128, 2 * half), 1) < half

    def turn_rows(index, most):
        at = pl.ds(pl.multiple_of(index * 128, 128), 128)
        wide = got_keys[at, :].astype(jnp.float32)
        here = table[at, :]
        swapped = pltpu.roll(here, half, 1)
        cosine = jnp.where(first, here, swapped)
        sine = jnp.where(first, -swapped, here)
        turned = wide * cosine + pltpu.roll(wide, half, 1) * sine
        table[at, :] = turned
        return jnp.maximum(most, jnp.max(jnp.abs(turned).reshape(16, 8, 2 * half), axis=0))

    most = lax.fori_loop(0, length // 128, turn_rows, jnp.zeros((8, 2 * half), jnp.float32))
    scale = jnp.max(most, axis=0, keepdims=True)
    scale_ref[...] = scale
    factor = 1.0 / scale

    def narrow_rows(index, carry):
        at = pl.ds(pl.multiple_of(index * 128, 128), 128)
        out_keys[at, :] = (table[at, :] * factor).astype(jnp.bfloat16)
        return carry

    lax.fori_loop(0, length // 128, narrow_rows, 0)

    own_values.wait()
    others(0).wait_send()
    others(1).wait_send()
    others(1).wait_recv()


def put_out(keys, values, scale, out_keys, out_values, out_scale, sem):
    copies = [pltpu.make_async_copy(scale, out_scale, sem.at[0])]
    half = keys.shape[0] // 2
    for index, (source, target) in enumerate(((keys, out_keys), (values, out_values))):
        for piece in range(2):
            at = pl.ds(piece * half, half)
            copies.append(
                pltpu.make_async_copy(source.at[at], target.at[at], sem.at[1 + 2 * index + piece])
            )
    for one in copies:
        one.start()
    for one in copies:
        one.wait()


def local(blocks, spans, fresh_keys, fresh_values, turn_angle):
    batch, rows, _, size = fresh_keys.shape
    length = batch * rows
    shapes = [
        jax.ShapeDtypeStruct((length, size), jnp.bfloat16),
        jax.ShapeDtypeStruct((length, size), jnp.bfloat16),
        jax.ShapeDtypeStruct((1, size), jnp.float32),
    ]
    results = pl.pallas_call(
        functools.partial(kernel, blocks, spans, rows),
        out_shape=shapes,
        in_specs=[pl.BlockSpec(memory_space=pltpu.HBM)] * 3,
        out_specs=[
            pl.BlockSpec(memory_space=pltpu.VMEM),
            pl.BlockSpec(memory_space=pl.ANY),
            pl.BlockSpec(memory_space=pltpu.VMEM),
        ],
        scratch_shapes=[
            pltpu.VMEM((length, size), jnp.bfloat16),
            pltpu.VMEM((size // 2, length), jnp.float32),
            pltpu.VMEM((length, size), jnp.float32),
            pltpu.SemaphoreType.DMA((2,)),
            pltpu.SemaphoreType.DMA((2,)),
            pltpu.SemaphoreType.DMA((3,)),
            *[pltpu.SemaphoreType.REGULAR] * 4,
        ],
        compiler_params=pltpu.CompilerParams(
            collective_id=0, has_side_effects=True, vmem_limit_bytes=32 << 20
        ),
    )(
        *(
            pltpu.with_memory_space_constraint(array, pltpu.HBM)
            for array in (
                fresh_keys.reshape(length, size),
                fresh_values.reshape(length, size),
                turn_angle.T,
            )
        )
    )
    keys, values, scale = pl.pallas_call(
        put_out,
        out_shape=shapes,
        in_specs=[pl.BlockSpec(memory_space=pl.ANY)] * 3,
        out_specs=[pl.BlockSpec(memory_space=pl.ANY)] * 3,
        scratch_shapes=[pltpu.SemaphoreType.DMA((5,))],
        compiler_params=pltpu.CompilerParams(vmem_limit_bytes=1 << 20),
    )(*results)
    return (
        keys.reshape(1, length, 1, size),
        values.reshape(1, length, 1, size),
        scale.reshape(1, 1, size),
    )


def solution(mesh):
    blocks, spans = mesh.shape["block"], mesh.shape["span"]
    return jax.shard_map(
        functools.partial(local, blocks, spans),
        mesh=mesh,
        in_specs=(
            P(None, ("block", "span"), "heads", None),
            P(None, ("block", "span"), "heads", None),
            P(),
        ),
        out_specs=(
            P(("block", "span"), None, "heads", None),
            P(("block", "span"), None, "heads", None),
            P(("block", "span"), "heads", None),
        ),
        check_vma=False,
    )
```

```python
import functools

import jax
import jax.numpy as jnp
from jax import lax
from jax.experimental import pallas as pl
from jax.experimental.pallas import tpu as pltpu
from jax.sharding import PartitionSpec as P

MESH = pl.DeviceIdType.MESH
DISTANCES = (3, 4, 2, 1)
AHEAD = ((1, 2, 3, 4), (1,))


def kernel(
    blocks, spans, rows,
    keys_ref, values_ref, angle_ref,
    out_keys, out_values, scale_ref,
    got_keys, angle, table, send_sem, recv_sem, own_sem, near, far, across,
):
    y, z, h = lax.axis_index("block"), lax.axis_index("span"), lax.axis_index("heads")
    core = lax.rem(h, 2)
    me = y * spans + z
    length = angle.shape[1]
    half = angle.shape[0]

    def part(ref, index):
        return ref.at[pl.ds(pl.multiple_of(index * rows, rows), rows)]

    def send(which, dy, dz):
        source, target = ((keys_ref, got_keys), (values_ref, out_values))[which]
        ty, tz = lax.rem(y + dy, blocks), lax.rem(z + dz + spans, spans)
        pltpu.make_async_remote_copy(
            src_ref=part(source, ty * spans + tz),
            dst_ref=part(target, me),
            send_sem=send_sem.at[which],
            recv_sem=recv_sem.at[which],
            device_id=(ty, tz, h),
            device_id_type=MESH,
        ).start()

    def others(which):
        source, target = ((keys_ref, got_keys), (values_ref, out_values))[which]
        count = (blocks * spans - 1) * rows
        return pltpu.make_async_remote_copy(
            src_ref=source.at[pl.ds(0, count)],
            dst_ref=target.at[pl.ds(0, count)],
            send_sem=send_sem.at[which],
            recv_sem=recv_sem.at[which],
            device_id=(lax.rem(y + 1, blocks), z, h),
            device_id_type=MESH,
        )

    def sides(distance):
        return (distance,) if 2 * distance == spans else (distance, -distance)

    def send_in_ring(which, distance):
        if distance in AHEAD[which]:
            for dz in sides(distance):
                send(which, 0, dz)

    angle_in = pltpu.make_async_copy(angle_ref, angle, own_sem.at[2])
    angle_in.start()

    span_next, span_last = (y, lax.rem(z + 1, spans), h), (y, lax.rem(z + spans - 1, spans), h)
    block_next, block_last = (lax.rem(y + 1, blocks), z, h), (lax.rem(y + blocks - 1, blocks), z, h)
    barrier = pltpu.get_barrier_semaphore()
    for neighbour in (span_next, span_last, block_next, block_last):
        pl.semaphore_signal(barrier, inc=1, device_id=neighbour, device_id_type=MESH)
    pl.semaphore_wait(barrier, 4)

    def pass_on(sems, devices):
        for index, device in enumerate(devices):
            pl.semaphore_signal(sems.at[index], inc=1, device_id=device, device_id_type=MESH)
        for index in range(len(devices)):
            pl.semaphore_wait(sems.at[index], 1)

    for which in range(2):
        send_in_ring(which, 1)
    pass_on(near, (span_next, span_last, block_next, block_last))
    for which in range(2):
        send_in_ring(which, 2)
    pass_on(far, ((y, lax.rem(z + 2, spans), h), (y, lax.rem(z + spans - 2, spans), h)))
    for which in range(2):
        for distance in range(3, spans // 2 + 1):
            send_in_ring(which, distance)
    pass_on(across, (block_next, block_last, (lax.rem(y + 2, blocks), z, h)))

    for which in range(2):
        for turn in range(blocks):
            for place, distance in enumerate(DISTANCES):
                for side, dz in enumerate(sides(distance)):
                    step = 2 * core + (turn + place + side)
                    if distance not in AHEAD[which]:
                        send(which, lax.rem(step, blocks), dz)
                    elif turn < blocks - 1:
                        send(which, lax.rem(step, blocks - 1) + 1, dz)
            if turn:
                send(which, (1, 3, 2)[turn - 1], 0)
    own_keys = pltpu.make_async_copy(part(keys_ref, me), part(got_keys, me), own_sem.at[0])
    own_values = pltpu.make_async_copy(part(values_ref, me), part(out_values, me), own_sem.at[1])
    own_keys.start()
    own_values.start()
    angle_in.wait()

    def fill(index, carry):
        start = pl.multiple_of(index * 128, 128)
        here = angle[:, pl.ds(start, 128)]
        both = jnp.concatenate([jnp.cos(here), jnp.sin(here)], axis=0)
        table[pl.ds(start, 128), :] = both.T
        return carry

    lax.fori_loop(0, length // 128, fill, 0)

    own_keys.wait()
    others(0).wait_recv()

    first = lax.broadcasted_iota(jnp.int32, (128, 2 * half), 1) < half

    def turn_rows(index, most):
        at = pl.ds(pl.multiple_of(index * 128, 128), 128)
        wide = got_keys[at, :].astype(jnp.float32)
        here = table[at, :]
        swapped = pltpu.roll(here, half, 1)
        cosine = jnp.where(first, here, swapped)
        sine = jnp.where(first, -swapped, here)
        turned = wide * cosine + pltpu.roll(wide, half, 1) * sine
        table[at, :] = turned
        return jnp.maximum(most, jnp.max(jnp.abs(turned).reshape(16, 8, 2 * half), axis=0))

    most = lax.fori_loop(0, length // 128, turn_rows, jnp.zeros((8, 2 * half), jnp.float32))
    scale = jnp.max(most, axis=0, keepdims=True)
    scale_ref[...] = scale
    factor = 1.0 / scale

    def narrow_rows(index, carry):
        at = pl.ds(pl.multiple_of(index * 128, 128), 128)
        out_keys[at, :] = (table[at, :] * factor).astype(jnp.bfloat16)
        return carry

    lax.fori_loop(0, length // 128, narrow_rows, 0)

    own_values.wait()
    others(0).wait_send()
    others(1).wait_send()
    others(1).wait_recv()


def put_out(keys, values, scale, out_keys, out_values, out_scale, sem):
    copies = [pltpu.make_async_copy(scale, out_scale, sem.at[0])]
    half = keys.shape[0] // 2
    for index, (source, target) in enumerate(((keys, out_keys), (values, out_values))):
        for piece in range(2):
            at = pl.ds(piece * half, half)
            copies.append(
                pltpu.make_async_copy(source.at[at], target.at[at], sem.at[1 + 2 * index + piece])
            )
    for one in copies:
        one.start()
    for one in copies:
        one.wait()


def local(blocks, spans, fresh_keys, fresh_values, turn_angle):
    batch, rows, _, size = fresh_keys.shape
    length = batch * rows
    shapes = [
        jax.ShapeDtypeStruct((length, size), jnp.bfloat16),
        jax.ShapeDtypeStruct((length, size), jnp.bfloat16),
        jax.ShapeDtypeStruct((1, size), jnp.float32),
    ]
    results = pl.pallas_call(
        functools.partial(kernel, blocks, spans, rows),
        out_shape=shapes,
        in_specs=[pl.BlockSpec(memory_space=pltpu.HBM)] * 3,
        out_specs=[
            pl.BlockSpec(memory_space=pltpu.VMEM),
            pl.BlockSpec(memory_space=pl.ANY),
            pl.BlockSpec(memory_space=pltpu.VMEM),
        ],
        scratch_shapes=[
            pltpu.VMEM((length, size), jnp.bfloat16),
            pltpu.VMEM((size // 2, length), jnp.float32),
            pltpu.VMEM((length, size), jnp.float32),
            pltpu.SemaphoreType.DMA((2,)),
            pltpu.SemaphoreType.DMA((2,)),
            pltpu.SemaphoreType.DMA((3,)),
            pltpu.SemaphoreType.REGULAR((4,)),
            pltpu.SemaphoreType.REGULAR((2,)),
            pltpu.SemaphoreType.REGULAR((3,)),
        ],
        compiler_params=pltpu.CompilerParams(
            collective_id=0, has_side_effects=True, vmem_limit_bytes=32 << 20
        ),
    )(
        *(
            pltpu.with_memory_space_constraint(array, pltpu.HBM)
            for array in (
                fresh_keys.reshape(length, size),
                fresh_values.reshape(length, size),
                turn_angle.T,
            )
        )
    )
    keys, values, scale = pl.pallas_call(
        put_out,
        out_shape=shapes,
        in_specs=[pl.BlockSpec(memory_space=pl.ANY)] * 3,
        out_specs=[pl.BlockSpec(memory_space=pl.ANY)] * 3,
        scratch_shapes=[pltpu.SemaphoreType.DMA((5,))],
        compiler_params=pltpu.CompilerParams(vmem_limit_bytes=1 << 20),
    )(*results)
    return (
        keys.reshape(1, length, 1, size),
        values.reshape(1, length, 1, size),
        scale.reshape(1, 1, size),
    )


def solution(mesh):
    blocks, spans = mesh.shape["block"], mesh.shape["span"]
    return jax.shard_map(
        functools.partial(local, blocks, spans),
        mesh=mesh,
        in_specs=(
            P(None, ("block", "span"), "heads", None),
            P(None, ("block", "span"), "heads", None),
            P(),
        ),
        out_specs=(
            P(("block", "span"), None, "heads", None),
            P(("block", "span"), None, "heads", None),
            P(("block", "span"), "heads", None),
        ),
        check_vma=False,
    )
```
